256 devices in a mesh: band: 64 (over x, z, core), dir: 4 (over y).
Axes of the slice: x: 4, y: 4, z: 8, core: 2. Of those that a mesh axis runs over, the one named last changes fastest.
Arguments:
- visibilities: bfloat16 [128, 32, 2, 256, 256], P('band', 'dir'), as said below
- sky_model: bfloat16 [128, 32, 2, 256, 256], P('band', 'dir')
- rfi_flags: int32 [128, 8, 8], P('band'), may hold values from 0 to 1, as said below
- destination: int32 [128], P('band'), may hold values from 0 to 127, as said below
Outputs:
- delivered: float32 [128, 32, 2, 256], P('band', 'dir')
- coefficients: float32 [9, 32, 2, 256], P(None, 'dir')
- norm_values: float32 [2, 2], replicated
The draws below stay inside these ranges and needn't reach their ends.
Inputs may be any that keep to these rules, and one draw needn't show every extreme that they name: `rfi_flags`: 1 marks a flagged baseline block; the share of flagged blocks tends to fall with the subband index. destination holds every row of 0 to 127 once. With the rows split into 64 aligned blocks of 2 rows, one row of block i goes to a row of block i + 1 and the other to a row of block i + 32, modulo 128 // 2. `visibilities`: visibilities follow the model under unknown station gains, with noise.
All inputs are finite; a program needn't handle non-finite values.
Results may differ from the reference program's by a relative error of at most 0.0003.
Values sent between devices are 32-bit elements; how exact they have to be, the bound alone decides.
No kernel may reach another device: no remote copies, remote signals or barrier semaphores. Data moves between devices by JAX's collectives and lax.ppermute only.
A program may use at most 128 MiB of HBM per device.

```python
import jax
import jax.numpy as jnp
from jax import lax

STATIONS = 256
DIRECTIONS = 32
BLOCK = 32
DEGREE = 8
SWEEPS = 4
ITERS = 2
SB_DEV = 2
SUBBANDS = 128


def band_pair(key, band_row):
    band_key = jax.random.fold_in(jax.random.fold_in(key, 11), band_row)
    model_key, noise_key, rough_key = jax.random.split(band_key, 3)
    shared = jax.random.normal(jax.random.fold_in(key, 23), (4, DIRECTIONS, STATIONS), jnp.float32)
    rough = jax.random.normal(rough_key, (2, DIRECTIONS, STATIONS), jnp.float32)
    abscissa = (2.0 * band_row.astype(jnp.float32) + 1.0) / SUBBANDS - 1.0
    sky_values = jax.random.normal(model_key, (DIRECTIONS, 2, STATIONS, STATIONS), jnp.float32)
    noise_level = 0.5
    amp_spread = 0.25
    amplitude = 1.0 + amp_spread * shared[0] + 0.15 * abscissa * shared[1] + 0.1 * rough[0]
    phase = 0.8 * shared[2] + 0.5 * abscissa * shared[3] + 0.2 * rough[1]
    gain_re = amplitude * jnp.cos(phase)
    gain_im = amplitude * jnp.sin(phase)
    model_re = sky_values[:, 0]
    model_im = sky_values[:, 1]
    twist_re = model_re * gain_re[:, None, :] + model_im * gain_im[:, None, :]
    twist_im = model_im * gain_re[:, None, :] - model_re * gain_im[:, None, :]
    noise = jax.random.normal(noise_key, (2, DIRECTIONS, STATIONS, STATIONS), jnp.float32)
    data_re = gain_re[:, :, None] * twist_re - gain_im[:, :, None] * twist_im + noise_level * noise[0]
    data_im = gain_re[:, :, None] * twist_im + gain_im[:, :, None] * twist_re + noise_level * noise[1]
    return (sky_values.astype(jnp.bfloat16), jnp.stack([data_re, data_im], axis=1).astype(jnp.bfloat16))


def draw_sky_model(key, part):

    def one_band(band_row):
        return band_pair(key, band_row)[0]
    return lax.map(one_band, jnp.arange(SUBBANDS))


def draw_visibilities(key, part):

    def one_band(band_row):
        return band_pair(key, band_row)[1]
    return lax.map(one_band, jnp.arange(SUBBANDS))


def draw_rfi_flags(key, part):
    band_rows = jnp.arange(SUBBANDS)
    threshold = 750 - 600 * band_rows // max(SUBBANDS - 1, 1)
    blocks = STATIONS // BLOCK
    random_ints = jax.random.randint(jax.random.fold_in(key, 5), (SUBBANDS, blocks, blocks), 0, 1000)
    return (random_ints < threshold[:, None, None]).astype(jnp.int32)


def draw_destination(key, part):
    block_count = SUBBANDS // SB_DEV
    half_count = block_count // 2
    base_key = jax.random.fold_in(key, 7)
    send_key, recv_key = jax.random.split(base_key)
    send_perm = jax.vmap(lambda one_key: jax.random.permutation(one_key, SB_DEV))(jax.random.split(send_key, block_count))
    recv_perm = jax.vmap(lambda one_key: jax.random.permutation(one_key, SB_DEV))(jax.random.split(recv_key, block_count))
    block_ids = jnp.arange(block_count)[:, None]
    slot_ids = jnp.arange(SB_DEV)[None, :]
    source_rows = block_ids * SB_DEV + send_perm
    target_block = jnp.where(slot_ids == 0, (block_ids + 1) % block_count, jnp.where(slot_ids == 1, (block_ids + half_count) % block_count, block_ids + 0 * slot_ids))
    target_slot = recv_perm[target_block, slot_ids + 0 * block_ids]
    target_rows = target_block * SB_DEV + target_slot
    result = jnp.zeros((SUBBANDS,), jnp.int32).at[source_rows.reshape(-1)].set(target_rows.reshape(-1).astype(jnp.int32))
    return result.astype(jnp.int32)


def setup_inputs(seed: int = 0) -> dict:
    streams_of = jax.random.split(jax.random.key(seed), 5)
    return {
        "visibilities": draw_visibilities(jax.random.fold_in(streams_of[4], 71), 0),
        "sky_model": draw_sky_model(jax.random.fold_in(streams_of[4], 71), 0),
        "rfi_flags": draw_rfi_flags(jax.random.fold_in(streams_of[4], 71), 0),
        "destination": draw_destination(jax.random.fold_in(streams_of[4], 71), 0),
    }


highest = lax.Precision.HIGHEST
penalty_share = 0.4

def block_weights(rfi_flags):
    blocks = rfi_flags.shape[-1]
    kept_blocks = (1 - rfi_flags).astype(jnp.float32)
    leading = kept_blocks.shape[:-2]
    spread = jnp.broadcast_to(kept_blocks[..., :, None, :, None], leading + (blocks, BLOCK, blocks, BLOCK))
    stations = blocks * BLOCK
    spread = spread.reshape(leading + (stations, stations))
    return spread * (1.0 - jnp.eye(stations, dtype=jnp.float32))

def operators(visibilities, sky_model, rfi_flags):
    baseline = block_weights(rfi_flags)[..., None, :, :]
    data_re = visibilities[..., 0, :, :].astype(jnp.float32)
    data_im = visibilities[..., 1, :, :].astype(jnp.float32)
    model_re = sky_model[..., 0, :, :].astype(jnp.float32)
    model_im = sky_model[..., 1, :, :].astype(jnp.float32)
    oper_re = baseline * (model_re * data_re + model_im * data_im)
    oper_im = baseline * (model_re * data_im - model_im * data_re)
    square = baseline * (model_re * model_re + model_im * model_im)
    return (jnp.stack([oper_re, oper_im], axis=-3), square)

def chebyshev(band_rows, band_total):
    abscissa = (2.0 * band_rows + 1.0) / band_total - 1.0
    cheb_terms = [jnp.ones_like(abscissa), abscissa]
    for degree in range(2, DEGREE + 1):
        cheb_terms.append(2.0 * abscissa * cheb_terms[-1] - cheb_terms[-2])
    return jnp.stack(cheb_terms[:DEGREE + 1], axis=0)

def stefcal(operator, square, gain_now, target, penalty):
    pen_term = penalty[..., None, None, None]
    for sweep_index in range(SWEEPS):
        products = jnp.einsum('...kapq,...kbq->...kabp', operator, gain_now, precision=highest)
        real_part = products[..., 0, 0, :] - products[..., 1, 1, :]
        imag_part = products[..., 0, 1, :] + products[..., 1, 0, :]
        numerator = jnp.stack([real_part, imag_part], axis=-2)
        magnitude = lax.optimization_barrier(jnp.sum(gain_now * gain_now, axis=-2))
        denominator = jnp.einsum('...kpq,...kq->...kp', square, magnitude, precision=highest)
        updated = (numerator + pen_term * target) / (denominator[..., None, :] + pen_term)
        gain_now = 0.5 * (updated + gain_now) if sweep_index % 2 == 1 else updated
    return gain_now

def per_band(band_items):
    vis_band, model_band, flag_band, gain_band, target_band, pen_band = band_items
    operator, square = operators(vis_band, model_band, flag_band)
    return stefcal(operator, square, gain_band, target_band, pen_band)

def reference(visibilities, sky_model, rfi_flags, destination):
    band_total = visibilities.shape[0]
    directions = visibilities.shape[1]
    stations = visibilities.shape[-1]
    blocks = rfi_flags.shape[-1]
    weights = (1.0 + lax.optimization_barrier(jnp.sum(1 - rfi_flags, axis=(1, 2))).astype(jnp.float32)) / (1.0 + blocks * blocks)
    penalty = penalty_share * stations * weights
    cheb_basis = chebyshev(jnp.arange(band_total).astype(jnp.float32), band_total)
    weighted = cheb_basis * weights[None, :]
    gram_matrix = jnp.dot(weighted, cheb_basis.T, precision=highest)
    factor = jnp.linalg.cholesky(gram_matrix)
    normalizer = directions * 2.0 * stations * gram_matrix[0, 0]
    ones_part = jnp.ones((band_total, directions, stations), jnp.float32)
    unit_gains = jnp.stack([ones_part, jnp.zeros_like(ones_part)], axis=2)
    gain_now = unit_gains
    consensus = unit_gains
    dual_var = jnp.zeros_like(unit_gains)
    row_weight = weights[:, None, None, None]
    norm_rows = []
    coefficients = None
    for iteration in range(ITERS):
        gain_now = lax.map(per_band, (visibilities, sky_model, rfi_flags, gain_now, consensus - dual_var, penalty))
        projection = jnp.einsum('cs,skap->ckap', weighted, gain_now + dual_var, precision=highest)
        flat_proj = projection.reshape(projection.shape[0], -1)
        coefficients = jax.scipy.linalg.cho_solve((factor, True), flat_proj).reshape(projection.shape)
        fresh_gains = jnp.einsum('cs,ckap->skap', cheb_basis, coefficients, precision=highest)
        dual_var = dual_var + gain_now - fresh_gains
        primal = jnp.sqrt(jnp.sum(row_weight * (gain_now - fresh_gains) ** 2) / normalizer)
        dual_norm = jnp.sqrt(jnp.sum(row_weight * (fresh_gains - consensus) ** 2) / normalizer)
        norm_rows.append(jnp.stack([primal, dual_norm]))
        consensus = fresh_gains
    delivered = jnp.zeros_like(gain_now).at[destination].set(gain_now)
    return (delivered, coefficients, jnp.stack(norm_rows))
```

```python
import jax
import jax.numpy as jnp
from jax import lax
from jax.experimental import pallas as pl
from jax.experimental.pallas import tpu as pltpu
from jax.sharding import Mesh
from jax.sharding import PartitionSpec as P

BLOCK = 32
DEGREE = 8
SWEEPS = 4
BAND = ("band_0", "band_1", "band_2")
LOCAL = 2
DIRS = 8
STATIONS = 256
PAIRS = LOCAL * DIRS
ORDER = DEGREE + 1
CHUNK = 8
MSG_ROWS = 8
USED_ROWS = 6

f32 = jnp.float32
highest = lax.Precision.HIGHEST
penalty_share = 0.4


def iota(shape, dim):
    return lax.broadcasted_iota(jnp.int32, shape, dim)


def dot(a, b):
    return jnp.dot(a, b, precision=highest, preferred_element_type=f32)


def total(x):
    return jnp.sum(jnp.sum(x, axis=1, keepdims=True), axis=0, keepdims=True)


def band_weights(flags_ref):
    blocks = flags_ref.shape[-1]
    keep = [1.0 - flags_ref[f].astype(f32) for f in range(LOCAL)]
    return keep, [(1.0 + total(one)) / (1.0 + blocks * blocks) for one in keep]


def penalty_rows(weights):
    row = iota((PAIRS, STATIONS), 0)
    return jnp.where(row < DIRS, *(penalty_share * STATIONS * w for w in weights))


def row_sums(col_ref, part, j, rows, value):
    lane = part * PAIRS + j
    col_ref[rows, lane : lane + 1] = jnp.sum(
        value[:, :128] + value[:, 128:], axis=1, keepdims=True
    )


def products(re_ref, im_ref, sq_ref, gain_ref, col_ref):
    for j in range(PAIRS):
        g_re = jnp.broadcast_to(gain_ref[j : j + 1, :], (CHUNK, STATIONS))
        g_im = jnp.broadcast_to(gain_ref[PAIRS + j : PAIRS + j + 1, :], (CHUNK, STATIONS))
        mag = g_re * g_re + g_im * g_im
        for start in range(0, STATIONS, CHUNK):
            rows = slice(start, start + CHUNK)
            a_re = re_ref[j, rows, :]
            a_im = im_ref[j, rows, :]
            row_sums(col_ref, 0, j, rows, a_re * g_re - a_im * g_im)
            row_sums(col_ref, 1, j, rows, a_re * g_im + a_im * g_re)
            row_sums(col_ref, 2, j, rows, sq_ref[j, rows, :] * mag)
    return jnp.transpose(col_ref[...])[: 3 * PAIRS]


def updated(sums, target_re, target_im, pen):
    scale = sums[2 * PAIRS :] + pen
    return (
        (sums[:PAIRS] + pen * target_re) / scale,
        (sums[PAIRS : 2 * PAIRS] + pen * target_im) / scale,
    )


def sweeps(first, refs, gain_ref, col_ref, target_re, target_im, pen):
    def sweep(index, carry):
        new_re, new_im = updated(
            products(*refs, gain_ref, col_ref), target_re, target_im, pen
        )
        odd = index % 2 == 1
        gain_ref[:PAIRS] = jnp.where(odd, 0.5 * (new_re + gain_ref[:PAIRS]), new_re)
        gain_ref[PAIRS:] = jnp.where(odd, 0.5 * (new_im + gain_ref[PAIRS:]), new_im)
        return carry

    lax.fori_loop(first, SWEEPS, sweep, 0)


def write_message(gain_ref, msg_ref, extras):
    low = iota((DIRS, 128), 1) < 64
    for f in range(LOCAL):
        for part in range(2):
            start = part * PAIRS + f * DIRS
            for quarter in range(4):
                tile = gain_ref[start : start + DIRS, 128 * (quarter // 2) : 128 * (quarter // 2) + 128]
                if quarter % 2:
                    tile = pltpu.roll(tile, 64, 1)
                if extras is not None:
                    tile = jnp.where(low, tile, extras[f])
                msg_ref[pl.ds(quarter * 32 + 2 * part + f, DIRS, stride=4), :] = tile


def first_kernel(
    flags_ref, dest_ref, vis_ref, sky_ref, re_ref, im_ref, sq_ref, gain_ref, msg_ref,
    vis_buf, sky_buf, mask_ref, col_ref, sems,
):
    def copies(j):
        f, k = j // DIRS, j % DIRS
        return (
            pltpu.make_async_copy(vis_ref.at[f, k], vis_buf.at[j], sems.at[0, j]),
            pltpu.make_async_copy(sky_ref.at[f, k], sky_buf.at[j], sems.at[1, j]),
        )

    for j in range(PAIRS):
        for copy in copies(j):
            copy.start()
    blocks = flags_ref.shape[-1]
    keep, weights = band_weights(flags_ref)
    spread = ((iota((STATIONS, blocks), 0) >> 5) == iota((STATIONS, blocks), 1)).astype(f32)
    across = ((iota((blocks, STATIONS), 1) >> 5) == iota((blocks, STATIONS), 0)).astype(f32)
    apart = iota((STATIONS, STATIONS), 0) != iota((STATIONS, STATIONS), 1)
    for f in range(LOCAL):
        mask_ref[f] = jnp.where(apart, dot(dot(spread, keep[f]), across), 0.0)
    col_ref[...] = jnp.zeros(col_ref.shape, f32)
    for j in range(PAIRS):
        for copy in copies(j):
            copy.wait()
        for start in range(0, STATIONS, 16):
            rows = slice(start, start + 16)
            mask = mask_ref[j // DIRS, rows, :]
            data_re = vis_buf[j, 0, rows, :].astype(f32)
            data_im = vis_buf[j, 1, rows, :].astype(f32)
            model_re = mask * sky_buf[j, 0, rows, :].astype(f32)
            model_im = mask * sky_buf[j, 1, rows, :].astype(f32)
            a_re = model_re * data_re + model_im * data_im
            a_im = model_re * data_im - model_im * data_re
            sq = model_re * model_re + model_im * model_im
            re_ref[j, rows, :] = a_re
            im_ref[j, rows, :] = a_im
            sq_ref[j, rows, :] = sq
            row_sums(col_ref, 0, j, rows, a_re)
            row_sums(col_ref, 1, j, rows, a_im)
            row_sums(col_ref, 2, j, rows, sq)
    pen = penalty_rows(weights)
    ones, zeros = jnp.ones((PAIRS, STATIONS), f32), jnp.zeros((PAIRS, STATIONS), f32)
    sums = jnp.transpose(col_ref[...])[: 3 * PAIRS]
    gain_ref[:PAIRS], gain_ref[PAIRS:] = updated(sums, ones, zeros, pen)
    sweeps(1, (re_ref, im_ref, sq_ref), gain_ref, col_ref, ones, zeros, pen)
    lane = iota((DIRS, 128), 1)
    extras = [
        jnp.where(lane < 96, weights[f], dest_ref[f].astype(f32)) for f in range(LOCAL)
    ]
    write_message(gain_ref, msg_ref, extras)


def second_kernel(
    flags_ref, re_ref, im_ref, sq_ref, start_ref, back_ref, msg_ref, gain_ref, target_ref, col_ref
):
    low = iota((DIRS, 128), 1) < 64
    for f in range(LOCAL):
        for part in range(2):
            start = part * PAIRS + f * DIRS
            for half in range(2):
                first, second = (
                    back_ref[pl.ds(quarter * 32 + 2 * part + f, DIRS, stride=4), :]
                    for quarter in (2 * half, 2 * half + 1)
                )
                target_ref[start : start + DIRS, 128 * half : 128 * half + 128] = jnp.where(
                    low, first, pltpu.roll(second, 64, 1)
                )
    col_ref[...] = jnp.zeros(col_ref.shape, f32)
    pen = penalty_rows(band_weights(flags_ref)[1])
    target_re, target_im = target_ref[:PAIRS], target_ref[PAIRS:]
    gain_ref[...] = start_ref[...]
    sweeps(0, (re_ref, im_ref, sq_ref), gain_ref, col_ref, target_re, target_im, pen)
    write_message(gain_ref, msg_ref, None)


def chebyshev(abscissa):
    terms = [jnp.ones_like(abscissa), abscissa]
    for _ in range(2, ORDER):
        terms.append(2.0 * abscissa * terms[-1] - terms[-2])
    return terms


def basis_columns(bands):
    row, lane = iota((bands, 128), 0), iota((bands, 128), 1)
    out = jnp.zeros((bands, 128), f32)
    for c, term in enumerate(chebyshev((2.0 * row.astype(f32) + 1.0) / bands - 1.0)):
        out = jnp.where(lane == c, term, out)
    return out


def basis_rows(bands):
    row, lane = iota((16, bands), 0), iota((16, bands), 1)
    out = jnp.zeros((16, bands), f32)
    for c, term in enumerate(chebyshev((2.0 * lane.astype(f32) + 1.0) / bands - 1.0)):
        out = jnp.where(row == c, term, out)
    return out


def solve_kernel(x_ref, msg_ref, fresh_ref, coef_ref, inverse_ref, norm_ref):
    bands = x_ref.shape[0]
    low = iota((bands, 128), 1) < 64
    gains = jnp.where(low, x_ref[...], 0.0)
    weight = x_ref[:, 64:65]
    columns, rows = basis_columns(bands), basis_rows(bands)
    coef = dot(rows, weight * gains)
    gram = dot(rows, weight * columns)
    row = iota((16, 128), 0)
    inverse = (row == iota((16, 128), 1)).astype(f32)
    for i in range(ORDER):
        scale = 1.0 / gram[i : i + 1, i : i + 1]
        factor = jnp.where(row == i, 0.0, gram[:, i : i + 1])
        pivots = [m[i : i + 1, :] * scale for m in (coef, gram, inverse)]
        coef, gram, inverse = (
            jnp.where(row == i, pivot, m - factor * pivot)
            for m, pivot in zip((coef, gram, inverse), pivots)
        )
    fresh = dot(columns[:, :16], coef)
    msg_ref[...] = 2.0 * fresh - gains
    fresh_ref[...] = fresh
    coef_ref[...] = coef
    inverse_ref[...] = inverse
    start = jnp.where(lax.axis_index("band_2") == 0, 1.0, 0.0)
    primal = total(weight * (gains - fresh) ** 2)
    dual = total(jnp.where(low, weight * (fresh - start) ** 2, 0.0))
    lane = iota((8, 128), 1)
    norm_ref[...] = jnp.where(
        lane == 64, primal, jnp.where(lane == 65, dual, jnp.where(lane == 68, total(weight), 0.0))
    )


def finish_kernel(
    x_ref, target_ref, gain_ref, fresh_ref, coef_ref, inverse_ref, norm_ref, msg_ref,
    coef_buf, rows_buf,
):
    bands = x_ref.shape[0]
    owners = bands // 2
    low = iota((bands, 128), 1) < 64
    weight = x_ref[:, 64:65]
    gains = jnp.where(low, gain_ref[...], 0.0)
    columns, rows = basis_columns(bands), basis_rows(bands)
    change = dot(inverse_ref[:, :16], dot(rows, weight * (gains - target_ref[...])))
    step = dot(columns[:, :16], change)
    fresh = fresh_ref[...] + step
    primal = total(weight * (gains - fresh) ** 2)
    dual = total(weight * step * step)
    lane = iota((8, 128), 1)
    norms = jnp.where(lane == 66, primal, jnp.where(lane == 67, dual, norm_ref[...]))
    row = iota((16, 128), 0)
    coef_buf[...] = jnp.where(
        row == ORDER, pltpu.roll(norms[:1], 64, 1), coef_ref[...] + change
    )
    low = iota((8, 128), 1) < 64
    packed = jnp.where(
        low, coef_buf[pl.ds(0, 8, stride=2), :], pltpu.roll(coef_buf[pl.ds(1, 8, stride=2), :], 64, 1)
    )
    for r in range(USED_ROWS - 1):
        msg_ref[pl.ds(r, owners, stride=MSG_ROWS), :] = jnp.broadcast_to(
            packed[r : r + 1], (owners, 128)
        )
    lands = (x_ref[:, 96:97] == iota((bands, bands), 1).astype(f32)).astype(f32)
    rows_buf[...] = dot(jnp.transpose(lands), gains)
    for r in range(USED_ROWS, MSG_ROWS):
        msg_ref[pl.ds(r, owners, stride=MSG_ROWS), :] = jnp.zeros((owners, 128), f32)
    msg_ref[pl.ds(USED_ROWS - 1, owners, stride=MSG_ROWS), :] = jnp.where(
        iota((owners, 128), 1) < 64,
        rows_buf[pl.ds(0, owners, stride=2), :],
        pltpu.roll(rows_buf[pl.ds(1, owners, stride=2), :], 64, 1),
    )


def assemble_kernel(all_ref, delivered_ref, coef_ref, norm_ref):
    owners = all_ref.shape[0] // MSG_ROWS
    low = iota((16, 128), 1) < 64
    for r in range(USED_ROWS):
        for half in range(2):
            first, second = (
                all_ref[pl.ds(MSG_ROWS * 16 * quarter + r, 16, stride=MSG_ROWS), :]
                for quarter in (2 * half, 2 * half + 1)
            )
            tiles = (
                jnp.where(low, first, pltpu.roll(second, 64, 1)),
                jnp.where(low, pltpu.roll(first, 64, 1), second),
            )
            for odd in range(2):
                if r == USED_ROWS - 1:
                    out = delivered_ref.at[odd]
                elif 2 * r + odd < ORDER:
                    out = coef_ref.at[2 * r + odd]
                else:
                    continue
                for k in range(DIRS):
                    out[k, :, 128 * half : 128 * half + 128] = tiles[odd][2 * k : 2 * k + 2]
    norm_ref[...] = jnp.broadcast_to(
        jnp.sum(all_ref[pl.ds(ORDER // 2, owners, stride=MSG_ROWS), :], axis=0, keepdims=True),
        norm_ref.shape,
    )


def shape(*dims):
    return jax.ShapeDtypeStruct(dims, f32)


def call(kernel, outs, *args, scratch=(), in_specs=None, limit=8 << 20):
    in_specs = in_specs or [VMEM] * len(args)
    args = [
        pltpu.with_memory_space_constraint(arg, spec.memory_space)
        for arg, spec in zip(args, in_specs)
    ]
    return pl.pallas_call(
        kernel,
        out_shape=outs,
        in_specs=in_specs,
        scratch_shapes=list(scratch),
        compiler_params=pltpu.CompilerParams(vmem_limit_bytes=limit),
        name=kernel.__name__,
    )(*args)


VMEM = pl.BlockSpec(memory_space=pltpu.VMEM)
SMEM = pl.BlockSpec(memory_space=pltpu.SMEM)
HBM = pl.BlockSpec(memory_space=pltpu.HBM)


def exchange(message):
    return lax.all_to_all(message, BAND, split_axis=0, concat_axis=0, tiled=True)


def per_device(visibilities, sky_model, rfi_flags, destination):
    bands = LOCAL * lax.axis_size(BAND)
    columns = pltpu.VMEM((STATIONS, 128), f32)
    operator = pltpu.VMEM((PAIRS, STATIONS, STATIONS), f32)
    halves = pltpu.VMEM((PAIRS, 2, STATIONS, STATIONS), jnp.bfloat16)
    re, im, sq, gains, message = call(
        first_kernel,
        [operator, operator, operator, shape(2 * PAIRS, STATIONS), shape(bands, 128)],
        rfi_flags, destination, visibilities, sky_model,
        in_specs=[VMEM, SMEM, HBM, HBM],
        scratch=[
            halves, halves, pltpu.VMEM((LOCAL, STATIONS, STATIONS), f32), columns,
            pltpu.SemaphoreType.DMA((2, PAIRS)),
        ],
        limit=20 << 20,
    )
    operators = (re, im, sq)
    held = exchange(message)
    target, fresh, coef, inverse, norms = call(
        solve_kernel,
        [shape(bands, 128), shape(bands, 128), shape(16, 128), shape(16, 128), shape(8, 128)],
        held,
    )
    back = exchange(target)
    rows = pltpu.VMEM((2 * PAIRS, STATIONS), f32)
    message = call(
        second_kernel, shape(bands, 128), rfi_flags, *operators, gains, back,
        scratch=[rows, rows, columns],
    )
    message = call(
        finish_kernel, shape(MSG_ROWS * bands // LOCAL, 128),
        held, target, exchange(message), fresh, coef, inverse, norms,
        scratch=[pltpu.VMEM((16, 128), f32), pltpu.VMEM((bands, 128), f32)],
    )
    delivered, coefficients, norms = call(
        assemble_kernel,
        [
            shape(LOCAL, DIRS, 2, STATIONS), shape(ORDER, DIRS, 2, STATIONS), shape(8, 128),
        ],
        exchange(message),
    )
    count = lax.axis_size("dir")
    others = [
        lax.ppermute(norms, "dir", [(i, i ^ bit) for i in range(count)]) for bit in (1, 2, 3)
    ]
    sums = (norms + others[0]) + (others[1] + others[2])
    normalizer = (DIRS * count * 2.0 * STATIONS) * (norms[0, 68] / (bands // LOCAL))
    norm_values = jnp.sqrt(sums[0, 64:68].reshape(2, 2) / normalizer)
    return delivered, coefficients, norm_values


def solution(mesh):
    finer = Mesh(
        mesh.devices.reshape(4, 8, 2, mesh.shape["dir"]), ("band_0", "band_1", "band_2", "dir")
    )
    return jax.shard_map(
        per_device,
        mesh=finer,
        in_specs=(
            P(BAND, "dir", None, None, None),
            P(BAND, "dir", None, None, None),
            P(BAND, None, None),
            P(BAND),
        ),
        out_specs=(P(BAND, "dir", None, None), P(None, "dir", None, None), P()),
        check_vma=False,
    )
```

```python
import jax
import jax.numpy as jnp
from jax import lax
from jax.experimental import pallas as pl
from jax.experimental.pallas import tpu as pltpu
from jax.sharding import Mesh
from jax.sharding import PartitionSpec as P

BLOCK = 32
DEGREE = 8
SWEEPS = 4
BAND = ("band_0", "band_1", "band_2")
LOCAL = 2
DIRS = 8
STATIONS = 256
PAIRS = LOCAL * DIRS
ORDER = DEGREE + 1
CHUNK = 8
MSG_ROWS = 6
AHEAD = 5

f32 = jnp.float32
bf16 = jnp.bfloat16
highest = lax.Precision.HIGHEST
penalty_share = 0.4


def iota(shape, dim):
    return lax.broadcasted_iota(jnp.int32, shape, dim)


def dot(a, b):
    return jnp.dot(a, b, precision=highest, preferred_element_type=f32)


def matrix_dot(a, b):
    return jnp.dot(a, b, preferred_element_type=f32)


def total(x):
    return jnp.sum(jnp.sum(x, axis=1, keepdims=True), axis=0, keepdims=True)


def band_weights(flags_ref):
    blocks = flags_ref.shape[-1]
    keep = [1.0 - flags_ref[f].astype(f32) for f in range(LOCAL)]
    return keep, [(1.0 + total(one)) / (1.0 + blocks * blocks) for one in keep]


def penalty_rows(weights):
    row = iota((PAIRS, STATIONS), 0)
    return jnp.where(row < DIRS, *(penalty_share * STATIONS * w for w in weights))


def row_sums(col_ref, part, j, rows, value):
    lane = part * PAIRS + j
    col_ref[rows, lane : lane + 1] = jnp.sum(
        value[:, :128] + value[:, 128:], axis=1, keepdims=True
    )


def products(re_ref, im_ref, sq_ref, gain_ref, col_ref):
    for j in range(PAIRS):
        g_re = jnp.broadcast_to(gain_ref[j : j + 1, :], (CHUNK, STATIONS))
        g_im = jnp.broadcast_to(gain_ref[PAIRS + j : PAIRS + j + 1, :], (CHUNK, STATIONS))
        mag = g_re * g_re + g_im * g_im
        for start in range(0, STATIONS, CHUNK):
            rows = slice(start, start + CHUNK)
            a_re = re_ref[j, rows, :]
            a_im = im_ref[j, rows, :]
            row_sums(col_ref, 0, j, rows, a_re * g_re - a_im * g_im)
            row_sums(col_ref, 1, j, rows, a_re * g_im + a_im * g_re)
            row_sums(col_ref, 2, j, rows, sq_ref[j, rows, :] * mag)
    return jnp.transpose(col_ref[...])[: 3 * PAIRS]


def updated(sums, target_re, target_im, pen):
    scale = sums[2 * PAIRS :] + pen
    return (
        (sums[:PAIRS] + pen * target_re) / scale,
        (sums[PAIRS : 2 * PAIRS] + pen * target_im) / scale,
    )


def sweeps(first, refs, gain_ref, col_ref, target_re, target_im, pen):
    def sweep(index, carry):
        new_re, new_im = updated(
            products(*refs, gain_ref, col_ref), target_re, target_im, pen
        )
        odd = index % 2 == 1
        gain_ref[:PAIRS] = jnp.where(odd, 0.5 * (new_re + gain_ref[:PAIRS]), new_re)
        gain_ref[PAIRS:] = jnp.where(odd, 0.5 * (new_im + gain_ref[PAIRS:]), new_im)
        return carry

    lax.fori_loop(first, SWEEPS, sweep, 0)


def write_message(gain_ref, msg_ref, extras):
    low = iota((DIRS, 128), 1) < 64
    for f in range(LOCAL):
        for part in range(2):
            start = part * PAIRS + f * DIRS
            for quarter in range(4):
                tile = gain_ref[start : start + DIRS, 128 * (quarter // 2) : 128 * (quarter // 2) + 128]
                if quarter % 2:
                    tile = pltpu.roll(tile, 64, 1)
                if extras is not None:
                    tile = jnp.where(low, tile, extras[f])
                msg_ref[pl.ds(quarter * 32 + 2 * part + f, DIRS, stride=4), :] = tile


def first_kernel(
    flags_in, dest_in, vis_ref, sky_ref, re_ref, im_ref, sq_ref, gain_ref, pen_ref, msg_ref,
    flags_ref, dest_ref, vis_buf, sky_buf, mask_ref, col_ref, sems,
):
    def copies(j):
        f, k = j // DIRS, j % DIRS
        return (
            pltpu.make_async_copy(vis_ref.at[f, k], vis_buf.at[j], sems.at[0, j]),
            pltpu.make_async_copy(sky_ref.at[f, k], sky_buf.at[j], sems.at[1, j]),
        )

    flags_copy = pltpu.make_async_copy(flags_in, flags_ref, sems.at[0, PAIRS])
    dest_copy = pltpu.make_async_copy(dest_in, dest_ref, sems.at[1, PAIRS])
    flags_copy.start()
    dest_copy.start()
    for j in range(AHEAD):
        for copy in copies(j):
            copy.start()
    flags_copy.wait()
    blocks = flags_ref.shape[-1]
    keep, weights = band_weights(flags_ref)
    spread = ((iota((STATIONS, blocks), 0) >> 5) == iota((STATIONS, blocks), 1)).astype(bf16)
    across = ((iota((blocks, STATIONS), 1) >> 5) == iota((blocks, STATIONS), 0)).astype(bf16)
    apart = iota((STATIONS, STATIONS), 0) != iota((STATIONS, STATIONS), 1)
    for f in range(LOCAL):
        wide = matrix_dot(matrix_dot(spread, keep[f].astype(bf16)).astype(bf16), across)
        mask_ref[f] = jnp.where(apart, wide, 0.0)
    col_ref[...] = jnp.zeros(col_ref.shape, f32)
    for j in range(PAIRS):
        for copy in copies(j):
            copy.wait()
        if j + AHEAD < PAIRS:
            for copy in copies(j + AHEAD):
                copy.start()
        for start in range(0, STATIONS, 16):
            rows = slice(start, start + 16)
            mask = mask_ref[j // DIRS, rows, :]
            data_re = vis_buf[j, 0, rows, :].astype(f32)
            data_im = vis_buf[j, 1, rows, :].astype(f32)
            model_re = mask * sky_buf[j, 0, rows, :].astype(f32)
            model_im = mask * sky_buf[j, 1, rows, :].astype(f32)
            a_re = model_re * data_re + model_im * data_im
            a_im = model_re * data_im - model_im * data_re
            sq = model_re * model_re + model_im * model_im
            re_ref[j, rows, :] = a_re
            im_ref[j, rows, :] = a_im
            sq_ref[j, rows, :] = sq
            row_sums(col_ref, 0, j, rows, a_re)
            row_sums(col_ref, 1, j, rows, a_im)
            row_sums(col_ref, 2, j, rows, sq)
    pen = penalty_rows(weights)
    pen_ref[...] = pen
    ones, zeros = jnp.ones((PAIRS, STATIONS), f32), jnp.zeros((PAIRS, STATIONS), f32)
    sums = jnp.transpose(col_ref[...])[: 3 * PAIRS]
    gain_ref[:PAIRS], gain_ref[PAIRS:] = updated(sums, ones, zeros, pen)
    sweeps(1, (re_ref, im_ref, sq_ref), gain_ref, col_ref, ones, zeros, pen)
    lane = iota((DIRS, 128), 1)
    dest_copy.wait()
    extras = [
        jnp.where(lane < 96, weights[f], dest_ref[f].astype(f32)) for f in range(LOCAL)
    ]
    write_message(gain_ref, msg_ref, extras)


def second_kernel(
    re_ref, im_ref, sq_ref, start_ref, pen_ref, back_ref, msg_ref, gain_ref, target_ref, col_ref
):
    low = iota((DIRS, 128), 1) < 64
    for f in range(LOCAL):
        for part in range(2):
            start = part * PAIRS + f * DIRS
            for half in range(2):
                first, second = (
                    back_ref[pl.ds(quarter * 32 + 2 * part + f, DIRS, stride=4), :]
                    for quarter in (2 * half, 2 * half + 1)
                )
                target_ref[start : start + DIRS, 128 * half : 128 * half + 128] = jnp.where(
                    low, first, pltpu.roll(second, 64, 1)
                )
    col_ref[...] = jnp.zeros(col_ref.shape, f32)
    pen = pen_ref[...]
    target_re, target_im = target_ref[:PAIRS], target_ref[PAIRS:]
    gain_ref[...] = start_ref[...]
    sweeps(0, (re_ref, im_ref, sq_ref), gain_ref, col_ref, target_re, target_im, pen)
    write_message(gain_ref, msg_ref, None)


def chebyshev(abscissa):
    terms = [jnp.ones_like(abscissa), abscissa]
    for _ in range(2, ORDER):
        terms.append(2.0 * abscissa * terms[-1] - terms[-2])
    return terms


def basis_columns(bands):
    row, lane = iota((bands, 128), 0), iota((bands, 128), 1)
    out = jnp.zeros((bands, 128), f32)
    for c, term in enumerate(chebyshev((2.0 * row.astype(f32) + 1.0) / bands - 1.0)):
        out = jnp.where(lane == c, term, out)
    return out


def basis_rows(bands):
    row, lane = iota((16, bands), 0), iota((16, bands), 1)
    out = jnp.zeros((16, bands), f32)
    for c, term in enumerate(chebyshev((2.0 * lane.astype(f32) + 1.0) / bands - 1.0)):
        out = jnp.where(row == c, term, out)
    return out


def solve_kernel(x_ref, msg_ref, fresh_ref, coef_ref, inverse_ref, norm_ref):
    bands = x_ref.shape[0]
    low = iota((bands, 128), 1) < 64
    gains = jnp.where(low, x_ref[...], 0.0)
    weight = x_ref[:, 64:65]
    columns, rows = basis_columns(bands), basis_rows(bands)
    coef = dot(rows, weight * gains)
    gram = dot(rows, weight * columns)
    row = iota((16, 128), 0)
    inverse = (row == iota((16, 128), 1)).astype(f32)
    for i in range(ORDER):
        scale = 1.0 / gram[i : i + 1, i : i + 1]
        factor = jnp.where(row == i, 0.0, gram[:, i : i + 1])
        pivots = [m[i : i + 1, :] * scale for m in (coef, gram, inverse)]
        coef, gram, inverse = (
            jnp.where(row == i, pivot, m - factor * pivot)
            for m, pivot in zip((coef, gram, inverse), pivots)
        )
    fresh = dot(columns[:, :16], coef)
    msg_ref[...] = 2.0 * fresh - gains
    fresh_ref[...] = fresh
    coef_ref[...] = coef
    inverse_ref[...] = inverse
    start = jnp.where(lax.axis_index("band_2") == 0, 1.0, 0.0)
    primal = total(weight * (gains - fresh) ** 2)
    dual = total(jnp.where(low, weight * (fresh - start) ** 2, 0.0))
    lane = iota((8, 128), 1)
    norm_ref[...] = jnp.where(
        lane == 64, primal, jnp.where(lane == 65, dual, jnp.where(lane == 68, total(weight), 0.0))
    )


def finish_kernel(
    x_ref, target_ref, gain_ref, fresh_ref, coef_ref, inverse_ref, norm_ref, msg_ref,
    coef_buf, rows_buf,
):
    bands = x_ref.shape[0]
    owners = bands // 2
    low = iota((bands, 128), 1) < 64
    weight = x_ref[:, 64:65]
    gains = jnp.where(low, gain_ref[...], 0.0)
    columns, rows = basis_columns(bands), basis_rows(bands)
    change = dot(inverse_ref[:, :16], dot(rows, weight * (gains - target_ref[...])))
    step = dot(columns[:, :16], change)
    fresh = fresh_ref[...] + step
    primal = total(weight * (gains - fresh) ** 2)
    dual = total(weight * step * step)
    lane = iota((8, 128), 1)
    norms = jnp.where(lane == 66, primal, jnp.where(lane == 67, dual, norm_ref[...]))
    row = iota((16, 128), 0)
    coef_buf[...] = jnp.where(
        row == ORDER, pltpu.roll(norms[:1], 64, 1), coef_ref[...] + change
    )
    low = iota((8, 128), 1) < 64
    packed = jnp.where(
        low, coef_buf[pl.ds(0, 8, stride=2), :], pltpu.roll(coef_buf[pl.ds(1, 8, stride=2), :], 64, 1)
    )
    for r in range(MSG_ROWS - 1):
        msg_ref[pl.ds(r, owners, stride=MSG_ROWS), :] = jnp.broadcast_to(
            packed[r : r + 1], (owners, 128)
        )
    lands = (x_ref[:, 96:97] == iota((bands, bands), 1).astype(f32)).astype(f32)
    rows_buf[...] = dot(jnp.transpose(lands), gains)
    msg_ref[pl.ds(MSG_ROWS - 1, owners, stride=MSG_ROWS), :] = jnp.where(
        iota((owners, 128), 1) < 64,
        rows_buf[pl.ds(0, owners, stride=2), :],
        pltpu.roll(rows_buf[pl.ds(1, owners, stride=2), :], 64, 1),
    )


def assemble_kernel(all_ref, delivered_ref, coef_ref):
    low = iota((16, 128), 1) < 64
    for r in range(MSG_ROWS):
        for half in range(2):
            first, second = (
                all_ref[pl.ds(MSG_ROWS * 16 * quarter + r, 16, stride=MSG_ROWS), :]
                for quarter in (2 * half, 2 * half + 1)
            )
            tiles = (
                jnp.where(low, first, pltpu.roll(second, 64, 1)),
                jnp.where(low, pltpu.roll(first, 64, 1), second),
            )
            for odd in range(2):
                if r == MSG_ROWS - 1:
                    out = delivered_ref.at[odd]
                elif 2 * r + odd < ORDER:
                    out = coef_ref.at[2 * r + odd]
                else:
                    continue
                for k in range(DIRS):
                    out[k, :, 128 * half : 128 * half + 128] = tiles[odd][2 * k : 2 * k + 2]


def norm_kernel(all_ref, norm_ref):
    owners = all_ref.shape[0] // MSG_ROWS
    sums = jnp.sum(all_ref[pl.ds(ORDER // 2, owners, stride=MSG_ROWS), :], axis=0, keepdims=True)
    sums = jnp.broadcast_to(sums, (8, 128))
    row = iota((8, 128), 0)
    norm_ref[...] = jnp.where(
        row == 0,
        pltpu.roll(sums, 64, 1),
        jnp.where(row == 1, pltpu.roll(sums, 62, 1), pltpu.roll(sums, 60, 1)),
    )


def total_kernel(own_ref, first_ref, second_ref, third_ref, out_ref):
    sums = (own_ref[...] + second_ref[...]) + (first_ref[...] + third_ref[...])
    scale = lax.axis_size(BAND) / (DIRS * lax.axis_size("dir") * 2.0 * STATIONS)
    out_ref[...] = jnp.sqrt(scale * sums[:2, :2] / own_ref[2:3, :1])


def shape(*dims):
    return jax.ShapeDtypeStruct(dims, f32)


def call(kernel, outs, *args, scratch=(), in_specs=None, limit=8 << 20):
    in_specs = in_specs or [VMEM] * len(args)
    args = [
        pltpu.with_memory_space_constraint(arg, spec.memory_space)
        for arg, spec in zip(args, in_specs)
    ]
    return pl.pallas_call(
        kernel,
        out_shape=outs,
        in_specs=in_specs,
        scratch_shapes=list(scratch),
        compiler_params=pltpu.CompilerParams(vmem_limit_bytes=limit),
        name=kernel.__name__,
    )(*args)


VMEM = pl.BlockSpec(memory_space=pltpu.VMEM)
HBM = pl.BlockSpec(memory_space=pltpu.HBM)


def exchange(message):
    return lax.all_to_all(message, BAND, split_axis=0, concat_axis=0, tiled=True)


def per_device(visibilities, sky_model, rfi_flags, destination):
    bands = LOCAL * lax.axis_size(BAND)
    columns = pltpu.VMEM((STATIONS, 128), f32)
    operator = pltpu.VMEM((PAIRS, STATIONS, STATIONS), f32)
    halves = pltpu.VMEM((PAIRS, 2, STATIONS, STATIONS), jnp.bfloat16)
    *state, message = call(
        first_kernel,
        [
            operator, operator, operator, shape(2 * PAIRS, STATIONS), shape(PAIRS, STATIONS),
            shape(bands, 128),
        ],
        rfi_flags, destination, visibilities, sky_model,
        in_specs=[HBM] * 4,
        scratch=[
            pltpu.VMEM(rfi_flags.shape, jnp.int32), pltpu.SMEM(destination.shape, jnp.int32),
            halves, halves, pltpu.VMEM((LOCAL, STATIONS, STATIONS), f32), columns,
            pltpu.SemaphoreType.DMA((2, PAIRS + 1)),
        ],
        limit=20 << 20,
    )
    held = exchange(message)
    target, fresh, coef, inverse, norms = call(
        solve_kernel,
        [shape(bands, 128), shape(bands, 128), shape(16, 128), shape(16, 128), shape(8, 128)],
        held,
    )
    back = exchange(target)
    rows = pltpu.VMEM((2 * PAIRS, STATIONS), f32)
    message = call(
        second_kernel, shape(bands, 128), *state, back,
        scratch=[rows, rows, columns],
    )
    message = call(
        finish_kernel, shape(MSG_ROWS * bands // LOCAL, 128),
        held, target, exchange(message), fresh, coef, inverse, norms,
        scratch=[pltpu.VMEM((16, 128), f32), pltpu.VMEM((bands, 128), f32)],
    )
    everything = exchange(message.reshape(bands // LOCAL, 1, MSG_ROWS * 128)).reshape(-1, 128)
    norms = call(norm_kernel, shape(8, 128), everything)
    count = lax.axis_size("dir")
    others = [
        lax.ppermute(norms, "dir", [(i, (i + step) % count) for i in range(count)])
        for step in range(1, count)
    ]
    delivered, coefficients = call(
        assemble_kernel,
        [shape(LOCAL, DIRS, 2, STATIONS), shape(ORDER, DIRS, 2, STATIONS)],
        everything,
    )
    norm_values = call(total_kernel, shape(2, 2), norms, *others)
    return delivered, coefficients, norm_values


def solution(mesh):
    finer = Mesh(
        mesh.devices.reshape(4, 8, 2, mesh.shape["dir"]), ("band_0", "band_1", "band_2", "dir")
    )
    return jax.shard_map(
        per_device,
        mesh=finer,
        in_specs=(
            P(BAND, "dir", None, None, None),
            P(BAND, "dir", None, None, None),
            P(BAND, None, None),
            P(BAND),
        ),
        out_specs=(P(BAND, "dir", None, None), P(None, "dir", None, None), P()),
        check_vma=False,
    )
```

```python
import jax
import jax.numpy as jnp
from jax import lax
from jax.experimental import pallas as pl
from jax.experimental.pallas import tpu as pltpu
from jax.sharding import Mesh
from jax.sharding import PartitionSpec as P

BLOCK = 32
DEGREE = 8
SWEEPS = 4
BAND = ("band_0", "band_1", "band_2")
LOCAL = 2
DIRS = 8
STATIONS = 256
PAIRS = LOCAL * DIRS
ORDER = DEGREE + 1
CHUNK = 8
MSG_ROWS = 6
AHEAD = 12
GROUP = 2

f32 = jnp.float32
bf16 = jnp.bfloat16
highest = lax.Precision.HIGHEST
penalty_share = 0.4


def iota(shape, dim):
    return lax.broadcasted_iota(jnp.int32, shape, dim)


def dot(a, b):
    return jnp.dot(a, b, precision=highest, preferred_element_type=f32)


def matrix_dot(a, b):
    return jnp.dot(a, b, preferred_element_type=f32)


def total(x):
    return jnp.sum(jnp.sum(x, axis=1, keepdims=True), axis=0, keepdims=True)


def band_weights(flags_ref):
    blocks = flags_ref.shape[-1]
    keep = [1.0 - flags_ref[f].astype(f32) for f in range(LOCAL)]
    return keep, [(1.0 + total(one)) / (1.0 + blocks * blocks) for one in keep]


def penalty_rows(weights):
    row = iota((PAIRS, STATIONS), 0)
    return jnp.where(row < DIRS, *(penalty_share * STATIONS * w for w in weights))


def row_sums(col_ref, part, j, rows, value):
    lane = part * PAIRS + j
    col_ref[rows, lane : lane + 1] = jnp.sum(
        value[:, :128] + value[:, 128:], axis=1, keepdims=True
    )


def products(re_ref, im_ref, sq_ref, gain_ref, col_ref):
    for j in range(PAIRS):
        g_re = jnp.broadcast_to(gain_ref[j : j + 1, :], (CHUNK, STATIONS))
        g_im = jnp.broadcast_to(gain_ref[PAIRS + j : PAIRS + j + 1, :], (CHUNK, STATIONS))
        mag = g_re * g_re + g_im * g_im
        for start in range(0, STATIONS, CHUNK):
            rows = slice(start, start + CHUNK)
            a_re = re_ref[j, rows, :]
            a_im = im_ref[j, rows, :]
            row_sums(col_ref, 0, j, rows, a_re * g_re - a_im * g_im)
            row_sums(col_ref, 1, j, rows, a_re * g_im + a_im * g_re)
            row_sums(col_ref, 2, j, rows, sq_ref[j, rows, :] * mag)
    return jnp.transpose(col_ref[...])[: 3 * PAIRS]


def updated(sums, target_re, target_im, pen):
    scale = sums[2 * PAIRS :] + pen
    return (
        (sums[:PAIRS] + pen * target_re) / scale,
        (sums[PAIRS : 2 * PAIRS] + pen * target_im) / scale,
    )


def sweeps(first, refs, gain_ref, col_ref, target_re, target_im, pen):
    def sweep(index, carry):
        new_re, new_im = updated(
            products(*refs, gain_ref, col_ref), target_re, target_im, pen
        )
        odd = index % 2 == 1
        gain_ref[:PAIRS] = jnp.where(odd, 0.5 * (new_re + gain_ref[:PAIRS]), new_re)
        gain_ref[PAIRS:] = jnp.where(odd, 0.5 * (new_im + gain_ref[PAIRS:]), new_im)
        return carry

    lax.fori_loop(first, SWEEPS, sweep, 0)


def quarters(ref, start):
    for quarter in range(4):
        tile = ref[start : start + DIRS, 128 * (quarter // 2) : 128 * (quarter // 2) + 128]
        yield quarter, (tile, pltpu.roll(tile, 64, 1))


def write_first(gain_ref, msg_ref, extras):
    low = iota((DIRS, 128), 1) < 64
    for f in range(LOCAL):
        for part in range(2):
            for quarter, tiles in quarters(gain_ref, part * PAIRS + f * DIRS):
                msg_ref[pl.ds(quarter * 32 + 2 * part + f, DIRS, stride=4), :] = jnp.where(
                    low, tiles[quarter % 2], extras[f]
                )


def write_packed(gain_ref, msg_ref):
    low = iota((DIRS, 128), 1) < 64
    for part in range(2):
        starts = (part * PAIRS, part * PAIRS + DIRS)
        for (quarter, one), (_, two) in zip(*(quarters(gain_ref, start) for start in starts)):
            msg_ref[pl.ds(quarter * 16 + part, DIRS, stride=2), :] = jnp.where(
                low, one[quarter % 2], two[1 - quarter % 2]
            )


def first_kernel(
    flags_in, dest_in, vis_ref, sky_ref, re_ref, im_ref, sq_ref, gain_ref, pen_ref, msg_ref,
    flags_ref, dest_ref, vis_buf, sky_buf, mask_ref, col_ref, sems,
):
    def copies(j):
        f, k = j // DIRS, j % DIRS
        return (
            pltpu.make_async_copy(vis_ref.at[f, k], vis_buf.at[j], sems.at[0, j]),
            pltpu.make_async_copy(sky_ref.at[f, k], sky_buf.at[j], sems.at[1, j]),
        )

    flags_copy = pltpu.make_async_copy(flags_in, flags_ref, sems.at[0, PAIRS])
    dest_copy = pltpu.make_async_copy(dest_in, dest_ref, sems.at[1, PAIRS])
    flags_copy.start()
    dest_copy.start()
    for j in range(AHEAD):
        for copy in copies(j):
            copy.start()
    flags_copy.wait()
    blocks = flags_ref.shape[-1]
    keep, weights = band_weights(flags_ref)
    spread = ((iota((STATIONS, blocks), 0) >> 5) == iota((STATIONS, blocks), 1)).astype(bf16)
    across = ((iota((blocks, STATIONS), 1) >> 5) == iota((blocks, STATIONS), 0)).astype(bf16)
    apart = iota((STATIONS, STATIONS), 0) != iota((STATIONS, STATIONS), 1)
    for f in range(LOCAL):
        wide = matrix_dot(matrix_dot(spread, keep[f].astype(bf16)).astype(bf16), across)
        mask_ref[f] = jnp.where(apart, wide, 0.0)
    col_ref[...] = jnp.zeros(col_ref.shape, f32)
    for j in range(PAIRS):
        if j % GROUP == 0:
            for i in range(j, j + GROUP):
                for copy in copies(i):
                    copy.wait()
            for i in range(j + AHEAD, min(j + AHEAD + GROUP, PAIRS)):
                for copy in copies(i):
                    copy.start()
        for start in range(0, STATIONS, 16):
            rows = slice(start, start + 16)
            mask = mask_ref[j // DIRS, rows, :]
            data_re = vis_buf[j, 0, rows, :].astype(f32)
            data_im = vis_buf[j, 1, rows, :].astype(f32)
            model_re = mask * sky_buf[j, 0, rows, :].astype(f32)
            model_im = mask * sky_buf[j, 1, rows, :].astype(f32)
            a_re = model_re * data_re + model_im * data_im
            a_im = model_re * data_im - model_im * data_re
            sq = model_re * model_re + model_im * model_im
            re_ref[j, rows, :] = a_re
            im_ref[j, rows, :] = a_im
            sq_ref[j, rows, :] = sq
            row_sums(col_ref, 0, j, rows, a_re)
            row_sums(col_ref, 1, j, rows, a_im)
            row_sums(col_ref, 2, j, rows, sq)
    pen = penalty_rows(weights)
    pen_ref[...] = pen
    ones, zeros = jnp.ones((PAIRS, STATIONS), f32), jnp.zeros((PAIRS, STATIONS), f32)
    sums = jnp.transpose(col_ref[...])[: 3 * PAIRS]
    gain_ref[:PAIRS], gain_ref[PAIRS:] = updated(sums, ones, zeros, pen)
    sweeps(1, (re_ref, im_ref, sq_ref), gain_ref, col_ref, ones, zeros, pen)
    lane = iota((DIRS, 128), 1)
    dest_copy.wait()
    extras = [
        jnp.where(lane < 96, weights[f], dest_ref[f].astype(f32)) for f in range(LOCAL)
    ]
    write_first(gain_ref, msg_ref, extras)


def second_kernel(
    re_ref, im_ref, sq_ref, start_ref, pen_ref, back_ref, msg_ref, gain_ref, target_ref, col_ref
):
    low = iota((DIRS, 128), 1) < 64
    for part in range(2):
        for half in range(2):
            first, second = (
                back_ref[pl.ds(quarter * 16 + part, DIRS, stride=2), :]
                for quarter in (2 * half, 2 * half + 1)
            )
            tiles = (
                jnp.where(low, first, pltpu.roll(second, 64, 1)),
                jnp.where(low, pltpu.roll(first, 64, 1), second),
            )
            for f in range(LOCAL):
                start = part * PAIRS + f * DIRS
                target_ref[start : start + DIRS, 128 * half : 128 * half + 128] = tiles[f]
    col_ref[...] = jnp.zeros(col_ref.shape, f32)
    pen = pen_ref[...]
    target_re, target_im = target_ref[:PAIRS], target_ref[PAIRS:]
    gain_ref[...] = start_ref[...]
    sweeps(0, (re_ref, im_ref, sq_ref), gain_ref, col_ref, target_re, target_im, pen)
    write_packed(gain_ref, msg_ref)


def chebyshev(abscissa):
    terms = [jnp.ones_like(abscissa), abscissa]
    for _ in range(2, ORDER):
        terms.append(2.0 * abscissa * terms[-1] - terms[-2])
    return terms


def basis_columns(bands):
    row, lane = iota((bands, 128), 0), iota((bands, 128), 1)
    out = jnp.zeros((bands, 128), f32)
    for c, term in enumerate(chebyshev((2.0 * row.astype(f32) + 1.0) / bands - 1.0)):
        out = jnp.where(lane == c, term, out)
    return out


def basis_rows(bands):
    row, lane = iota((16, bands), 0), iota((16, bands), 1)
    out = jnp.zeros((16, bands), f32)
    for c, term in enumerate(chebyshev((2.0 * lane.astype(f32) + 1.0) / bands - 1.0)):
        out = jnp.where(row == c, term, out)
    return out


def solve_kernel(
    x_ref, msg_ref, target_ref, fresh_ref, coef_ref, solver_ref, norm_ref
):
    bands = x_ref.shape[0]
    low = iota((bands, 128), 1) < 64
    gains = jnp.where(low, x_ref[...], 0.0)
    weight = x_ref[:, 64:65]
    columns, rows = basis_columns(bands), basis_rows(bands)
    coef = dot(rows, weight * gains)
    gram = dot(rows, weight * columns)
    row = iota((16, 128), 0)
    solved = (coef, gram, rows)
    for i in range(0, ORDER, 2):
        size = min(2, ORDER - i)
        picked = [
            jnp.broadcast_to(solved[1][:, i + n : i + n + 1], row.shape) for n in range(size)
        ]
        block = [[col[i + m : i + m + 1] for col in picked] for m in range(size)]
        if size == 1:
            inverse = [[1.0 / block[0][0]]]
        else:
            (p, q), (r, s) = block
            scale = 1.0 / (p * s - q * r)
            inverse = [[s * scale, -q * scale], [-r * scale, p * scale]]
        inside = (row >= i) & (row < i + size)
        factors = [jnp.where(inside, 0.0, col) for col in picked]
        after = []
        for m in solved:
            pivots = [sum(inverse[a][n] * m[i + n : i + n + 1] for n in range(size)) for a in range(size)]
            left = m - sum(factor * pivot for factor, pivot in zip(factors, pivots))
            for n, pivot in enumerate(pivots):
                left = jnp.where(row == i + n, pivot, left)
            after.append(left)
        solved = tuple(after)
    coef, _, solver = solved
    fresh = dot(columns[:, :16], coef)
    target_ref[...] = 2.0 * fresh - gains
    owners = bands // LOCAL
    msg_ref[...] = jnp.where(
        iota((owners, 128), 1) < 64,
        target_ref[pl.ds(0, owners, stride=2), :],
        pltpu.roll(target_ref[pl.ds(1, owners, stride=2), :], 64, 1),
    )
    fresh_ref[...] = fresh
    coef_ref[...] = coef
    solver_ref[...] = solver
    start = jnp.where(lax.axis_index("band_2") == 0, 1.0, 0.0)
    primal = total(weight * (gains - fresh) ** 2)
    dual = total(jnp.where(low, weight * (fresh - start) ** 2, 0.0))
    lane = iota((8, 128), 1)
    norm_ref[...] = jnp.where(
        lane == 64, primal, jnp.where(lane == 65, dual, jnp.where(lane == 68, total(weight), 0.0))
    )


def finish_kernel(
    x_ref, target_ref, gain_ref, fresh_ref, coef_ref, solver_ref, norm_ref, msg_ref,
    coef_buf, rows_buf, gain_buf,
):
    bands = x_ref.shape[0]
    owners = bands // 2
    low = iota((bands, 128), 1) < 64
    weight = x_ref[:, 64:65]
    gain_buf[pl.ds(0, owners, stride=2), :] = gain_ref[...]
    gain_buf[pl.ds(1, owners, stride=2), :] = pltpu.roll(gain_ref[...], 64, 1)
    gains = jnp.where(low, gain_buf[...], 0.0)
    columns = basis_columns(bands)
    change = dot(solver_ref[...], weight * (gains - target_ref[...]))
    step = dot(columns[:, :16], change)
    fresh = fresh_ref[...] + step
    primal = total(weight * (gains - fresh) ** 2)
    dual = total(weight * step * step)
    lane = iota((8, 128), 1)
    norms = jnp.where(lane == 66, primal, jnp.where(lane == 67, dual, norm_ref[...]))
    row = iota((16, 128), 0)
    coef_buf[...] = jnp.where(
        row == ORDER, pltpu.roll(norms[:1], 64, 1), coef_ref[...] + change
    )
    low = iota((8, 128), 1) < 64
    packed = jnp.where(
        low, coef_buf[pl.ds(0, 8, stride=2), :], pltpu.roll(coef_buf[pl.ds(1, 8, stride=2), :], 64, 1)
    )
    for r in range(MSG_ROWS - 1):
        msg_ref[pl.ds(r, owners, stride=MSG_ROWS), :] = jnp.broadcast_to(
            packed[r : r + 1], (owners, 128)
        )
    lands = (x_ref[:, 96:97] == iota((bands, bands), 1).astype(f32)).astype(f32)
    rows_buf[...] = dot(jnp.transpose(lands), gains)
    msg_ref[pl.ds(MSG_ROWS - 1, owners, stride=MSG_ROWS), :] = jnp.where(
        iota((owners, 128), 1) < 64,
        rows_buf[pl.ds(0, owners, stride=2), :],
        pltpu.roll(rows_buf[pl.ds(1, owners, stride=2), :], 64, 1),
    )


def assemble_kernel(all_ref, delivered_ref, coef_ref):
    low = iota((16, 128), 1) < 64
    for r in range(MSG_ROWS):
        for half in range(2):
            first, second = (
                all_ref[pl.ds(MSG_ROWS * 16 * quarter + r, 16, stride=MSG_ROWS), :]
                for quarter in (2 * half, 2 * half + 1)
            )
            tiles = (
                jnp.where(low, first, pltpu.roll(second, 64, 1)),
                jnp.where(low, pltpu.roll(first, 64, 1), second),
            )
            for odd in range(2):
                if r == MSG_ROWS - 1:
                    out = delivered_ref.at[odd]
                elif 2 * r + odd < ORDER:
                    out = coef_ref.at[2 * r + odd]
                else:
                    continue
                for k in range(DIRS):
                    out[k, :, 128 * half : 128 * half + 128] = tiles[odd][2 * k : 2 * k + 2]


def norm_kernel(all_ref, norm_ref):
    owners = all_ref.shape[0] // MSG_ROWS
    sums = jnp.sum(all_ref[pl.ds(ORDER // 2, owners, stride=MSG_ROWS), :], axis=0, keepdims=True)
    sums = jnp.broadcast_to(sums, (8, 128))
    row = iota((8, 128), 0)
    norm_ref[...] = jnp.where(
        row == 0,
        pltpu.roll(sums, 64, 1),
        jnp.where(row == 1, pltpu.roll(sums, 62, 1), pltpu.roll(sums, 60, 1)),
    )


def total_kernel(own_ref, first_ref, second_ref, third_ref, out_ref):
    sums = (own_ref[...] + second_ref[...]) + (first_ref[...] + third_ref[...])
    scale = lax.axis_size(BAND) / (DIRS * lax.axis_size("dir") * 2.0 * STATIONS)
    out_ref[...] = jnp.sqrt(scale * sums[:2, :2] / own_ref[2:3, :1])


def shape(*dims):
    return jax.ShapeDtypeStruct(dims, f32)


def call(kernel, outs, *args, scratch=(), in_specs=None, limit=8 << 20):
    in_specs = in_specs or [VMEM] * len(args)
    args = [
        pltpu.with_memory_space_constraint(arg, spec.memory_space)
        for arg, spec in zip(args, in_specs)
    ]
    return pl.pallas_call(
        kernel,
        out_shape=outs,
        in_specs=in_specs,
        scratch_shapes=list(scratch),
        compiler_params=pltpu.CompilerParams(vmem_limit_bytes=limit),
        name=kernel.__name__,
    )(*args)


VMEM = pl.BlockSpec(memory_space=pltpu.VMEM)
HBM = pl.BlockSpec(memory_space=pltpu.HBM)


def exchange(message):
    return lax.all_to_all(message, BAND, split_axis=0, concat_axis=0, tiled=True)


def per_device(visibilities, sky_model, rfi_flags, destination):
    bands = LOCAL * lax.axis_size(BAND)
    columns = pltpu.VMEM((STATIONS, 128), f32)
    operator = pltpu.VMEM((PAIRS, STATIONS, STATIONS), f32)
    halves = pltpu.VMEM((PAIRS, 2, STATIONS, STATIONS), jnp.bfloat16)
    *state, message = call(
        first_kernel,
        [
            operator, operator, operator, shape(2 * PAIRS, STATIONS), shape(PAIRS, STATIONS),
            shape(bands, 128),
        ],
        rfi_flags, destination, visibilities, sky_model,
        in_specs=[HBM] * 4,
        scratch=[
            pltpu.VMEM(rfi_flags.shape, jnp.int32), pltpu.SMEM(destination.shape, jnp.int32),
            halves, halves, pltpu.VMEM((LOCAL, STATIONS, STATIONS), f32), columns,
            pltpu.SemaphoreType.DMA((2, PAIRS + 1)),
        ],
        limit=20 << 20,
    )
    held = exchange(message)
    owners = bands // LOCAL
    message, *kept = call(
        solve_kernel,
        [
            shape(owners, 128), shape(bands, 128), shape(bands, 128), shape(16, 128),
            shape(16, 128), shape(8, 128),
        ],
        held,
    )
    rows = pltpu.VMEM((2 * PAIRS, STATIONS), f32)
    message = call(
        second_kernel, shape(owners, 128), *state, exchange(message),
        scratch=[rows, rows, columns],
    )
    target, *kept = kept
    spread = pltpu.VMEM((bands, 128), f32)
    message = call(
        finish_kernel, shape(MSG_ROWS * owners, 128), held, target, exchange(message), *kept,
        scratch=[pltpu.VMEM((16, 128), f32), spread, spread],
    )
    everything = exchange(message.reshape(owners, 1, MSG_ROWS * 128)).reshape(-1, 128)
    norms = call(norm_kernel, shape(8, 128), everything)
    count = lax.axis_size("dir")
    others = [
        lax.ppermute(norms, "dir", [(i, (i + step) % count) for i in range(count)])
        for step in range(1, count)
    ]
    delivered, coefficients = call(
        assemble_kernel,
        [shape(LOCAL, DIRS, 2, STATIONS), shape(ORDER, DIRS, 2, STATIONS)],
        everything,
    )
    norm_values = call(total_kernel, shape(2, 2), norms, *others)
    return delivered, coefficients, norm_values


def solution(mesh):
    finer = Mesh(
        mesh.devices.reshape(4, 8, 2, mesh.shape["dir"]), ("band_0", "band_1", "band_2", "dir")
    )
    return jax.shard_map(
        per_device,
        mesh=finer,
        in_specs=(
            P(BAND, "dir", None, None, None),
            P(BAND, "dir", None, None, None),
            P(BAND, None, None),
            P(BAND),
        ),
        out_specs=(P(BAND, "dir", None, None), P(None, "dir", None, None), P()),
        check_vma=False,
    )
```

```python
import jax
import jax.numpy as jnp
from jax import lax
from jax.experimental import pallas as pl
from jax.experimental.pallas import tpu as pltpu
from jax.sharding import Mesh
from jax.sharding import PartitionSpec as P

BLOCK = 32
DEGREE = 8
SWEEPS = 4
BAND = ("band_0", "band_1", "band_2")
LOCAL = 2
DIRS = 8
STATIONS = 256
PAIRS = LOCAL * DIRS
ORDER = DEGREE + 1
CHUNK = 8
MSG_ROWS = 6
GROUP = 2

f32 = jnp.float32
bf16 = jnp.bfloat16
highest = lax.Precision.HIGHEST
penalty_share = 0.4


def iota(shape, dim):
    return lax.broadcasted_iota(jnp.int32, shape, dim)


def dot(a, b):
    return jnp.dot(a, b, precision=highest, preferred_element_type=f32)


def matrix_dot(a, b):
    return jnp.dot(a, b, preferred_element_type=f32)


def total(x):
    return jnp.sum(jnp.sum(x, axis=1, keepdims=True), axis=0, keepdims=True)


def band_weights(flags_ref):
    blocks = flags_ref.shape[-1]
    keep = [1.0 - flags_ref[f].astype(f32) for f in range(LOCAL)]
    return keep, [(1.0 + total(one)) / (1.0 + blocks * blocks) for one in keep]


def penalty_rows(weights):
    row = iota((PAIRS, STATIONS), 0)
    return jnp.where(row < DIRS, *(penalty_share * STATIONS * w for w in weights))


def row_sums(col_ref, part, j, rows, value):
    lane = part * PAIRS + j
    col_ref[rows, lane : lane + 1] = jnp.sum(
        value[:, :128] + value[:, 128:], axis=1, keepdims=True
    )


def products(re_ref, im_ref, sq_ref, gain_ref, col_ref):
    for j in range(PAIRS):
        g_re = jnp.broadcast_to(gain_ref[j : j + 1, :], (CHUNK, STATIONS))
        g_im = jnp.broadcast_to(gain_ref[PAIRS + j : PAIRS + j + 1, :], (CHUNK, STATIONS))
        mag = g_re * g_re + g_im * g_im
        for start in range(0, STATIONS, CHUNK):
            rows = slice(start, start + CHUNK)
            a_re = re_ref[j, rows, :]
            a_im = im_ref[j, rows, :]
            row_sums(col_ref, 0, j, rows, a_re * g_re - a_im * g_im)
            row_sums(col_ref, 1, j, rows, a_re * g_im + a_im * g_re)
            row_sums(col_ref, 2, j, rows, sq_ref[j, rows, :] * mag)
    return jnp.transpose(col_ref[...])[: 3 * PAIRS]


def updated(sums, target_re, target_im, pen):
    scale = sums[2 * PAIRS :] + pen
    return (
        (sums[:PAIRS] + pen * target_re) / scale,
        (sums[PAIRS : 2 * PAIRS] + pen * target_im) / scale,
    )


def sweeps(first, refs, gain_ref, col_ref, target_re, target_im, pen):
    def sweep(index, carry):
        new_re, new_im = updated(
            products(*refs, gain_ref, col_ref), target_re, target_im, pen
        )
        odd = index % 2 == 1
        gain_ref[:PAIRS] = jnp.where(odd, 0.5 * (new_re + gain_ref[:PAIRS]), new_re)
        gain_ref[PAIRS:] = jnp.where(odd, 0.5 * (new_im + gain_ref[PAIRS:]), new_im)
        return carry

    lax.fori_loop(first, SWEEPS, sweep, 0)


def quarters(ref, start):
    for quarter in range(4):
        tile = ref[start : start + DIRS, 128 * (quarter // 2) : 128 * (quarter // 2) + 128]
        yield quarter, (tile, pltpu.roll(tile, 64, 1))


def write_first(gain_ref, msg_ref, extras):
    low = iota((DIRS, 128), 1) < 64
    for f in range(LOCAL):
        for part in range(2):
            for quarter, tiles in quarters(gain_ref, part * PAIRS + f * DIRS):
                msg_ref[pl.ds(quarter * 32 + 2 * part + f, DIRS, stride=4), :] = jnp.where(
                    low, tiles[quarter % 2], extras[f]
                )


def write_packed(gain_ref, msg_ref):
    low = iota((DIRS, 128), 1) < 64
    for part in range(2):
        starts = (part * PAIRS, part * PAIRS + DIRS)
        for (quarter, one), (_, two) in zip(*(quarters(gain_ref, start) for start in starts)):
            msg_ref[pl.ds(quarter * 16 + part, DIRS, stride=2), :] = jnp.where(
                low, one[quarter % 2], two[1 - quarter % 2]
            )


def first_kernel(
    flags_in, dest_in, vis_ref, sky_ref, re_ref, im_ref, sq_ref, gain_ref, pen_ref, msg_ref,
    flags_ref, dest_ref, vis_buf, sky_buf, mask_ref, col_ref, sems,
):
    def copies(j):
        f, k = j // DIRS, j % DIRS
        return (
            pltpu.make_async_copy(vis_ref.at[f, k], vis_buf.at[j], sems.at[0, j]),
            pltpu.make_async_copy(sky_ref.at[f, k], sky_buf.at[j], sems.at[1, j]),
        )

    flags_copy = pltpu.make_async_copy(flags_in, flags_ref, sems.at[0, PAIRS])
    dest_copy = pltpu.make_async_copy(dest_in, dest_ref, sems.at[1, PAIRS])
    flags_copy.start()
    dest_copy.start()
    for j in range(PAIRS):
        for copy in copies(j):
            copy.start()
    flags_copy.wait()
    blocks = flags_ref.shape[-1]
    keep, weights = band_weights(flags_ref)
    spread = ((iota((STATIONS, blocks), 0) >> 5) == iota((STATIONS, blocks), 1)).astype(bf16)
    across = ((iota((blocks, STATIONS), 1) >> 5) == iota((blocks, STATIONS), 0)).astype(bf16)
    apart = iota((STATIONS, STATIONS), 0) != iota((STATIONS, STATIONS), 1)
    for f in range(LOCAL):
        wide = matrix_dot(matrix_dot(spread, keep[f].astype(bf16)).astype(bf16), across)
        mask_ref[f] = jnp.where(apart, wide, 0.0).astype(bf16)
    col_ref[...] = jnp.zeros(col_ref.shape, f32)
    for j in range(PAIRS):
        if j < GROUP or j % GROUP == 0:
            for i in range(j, j + (1 if j < GROUP else GROUP)):
                for copy in copies(i):
                    copy.wait()
        for start in range(0, STATIONS, 16):
            rows = slice(start, start + 16)
            mask = mask_ref[j // DIRS, rows, :]
            data_re = vis_buf[j, 0, rows, :].astype(f32)
            data_im = vis_buf[j, 1, rows, :].astype(f32)
            model_re = (mask * sky_buf[j, 0, rows, :]).astype(f32)
            model_im = (mask * sky_buf[j, 1, rows, :]).astype(f32)
            a_re = model_re * data_re + model_im * data_im
            a_im = model_re * data_im - model_im * data_re
            sq = model_re * model_re + model_im * model_im
            re_ref[j, rows, :] = a_re
            im_ref[j, rows, :] = a_im
            sq_ref[j, rows, :] = sq
            row_sums(col_ref, 0, j, rows, a_re)
            row_sums(col_ref, 1, j, rows, a_im)
            row_sums(col_ref, 2, j, rows, sq)
    pen = penalty_rows(weights)
    pen_ref[...] = pen
    ones, zeros = jnp.ones((PAIRS, STATIONS), f32), jnp.zeros((PAIRS, STATIONS), f32)
    sums = jnp.transpose(col_ref[...])[: 3 * PAIRS]
    gain_ref[:PAIRS], gain_ref[PAIRS:] = updated(sums, ones, zeros, pen)
    sweeps(1, (re_ref, im_ref, sq_ref), gain_ref, col_ref, ones, zeros, pen)
    lane = iota((DIRS, 128), 1)
    dest_copy.wait()
    extras = [
        jnp.where(lane < 96, weights[f], dest_ref[f].astype(f32)) for f in range(LOCAL)
    ]
    write_first(gain_ref, msg_ref, extras)


def second_kernel(
    re_ref, im_ref, sq_ref, start_ref, pen_ref, back_ref, msg_ref, gain_ref, target_ref, col_ref
):
    low = iota((DIRS, 128), 1) < 64
    for part in range(2):
        for half in range(2):
            first, second = (
                back_ref[pl.ds(quarter * 16 + part, DIRS, stride=2), :]
                for quarter in (2 * half, 2 * half + 1)
            )
            tiles = (
                jnp.where(low, first, pltpu.roll(second, 64, 1)),
                jnp.where(low, pltpu.roll(first, 64, 1), second),
            )
            for f in range(LOCAL):
                start = part * PAIRS + f * DIRS
                target_ref[start : start + DIRS, 128 * half : 128 * half + 128] = tiles[f]
    col_ref[...] = jnp.zeros(col_ref.shape, f32)
    pen = pen_ref[...]
    target_re, target_im = target_ref[:PAIRS], target_ref[PAIRS:]
    gain_ref[...] = start_ref[...]
    sweeps(0, (re_ref, im_ref, sq_ref), gain_ref, col_ref, target_re, target_im, pen)
    write_packed(gain_ref, msg_ref)


def chebyshev(abscissa):
    terms = [jnp.ones_like(abscissa), abscissa]
    for _ in range(2, ORDER):
        terms.append(2.0 * abscissa * terms[-1] - terms[-2])
    return terms


def basis_columns(bands):
    row, lane = iota((bands, 128), 0), iota((bands, 128), 1)
    out = jnp.zeros((bands, 128), f32)
    for c, term in enumerate(chebyshev((2.0 * row.astype(f32) + 1.0) / bands - 1.0)):
        out = jnp.where(lane == c, term, out)
    return out


def basis_rows(bands):
    row, lane = iota((16, bands), 0), iota((16, bands), 1)
    out = jnp.zeros((16, bands), f32)
    for c, term in enumerate(chebyshev((2.0 * lane.astype(f32) + 1.0) / bands - 1.0)):
        out = jnp.where(row == c, term, out)
    return out


def solve_kernel(
    x_ref, msg_ref, target_ref, fresh_ref, coef_ref, solver_ref, norm_ref
):
    bands = x_ref.shape[0]
    low = iota((bands, 128), 1) < 64
    gains = jnp.where(low, x_ref[...], 0.0)
    weight = x_ref[:, 64:65]
    columns, rows = basis_columns(bands), basis_rows(bands)
    both = dot(rows, weight * jnp.concatenate([gains, columns], axis=1))
    coef, gram = both[:, :128], both[:, 128:]
    row = iota((16, 128), 0)
    solved = (coef, gram, rows)
    for i in range(0, ORDER, 2):
        size = min(2, ORDER - i)
        picked = [
            jnp.broadcast_to(solved[1][:, i + n : i + n + 1], row.shape) for n in range(size)
        ]
        block = [[col[i + m : i + m + 1] for col in picked] for m in range(size)]
        if size == 1:
            inverse = [[1.0 / block[0][0]]]
        else:
            (p, q), (r, s) = block
            scale = 1.0 / (p * s - q * r)
            inverse = [[s * scale, -q * scale], [-r * scale, p * scale]]
        inside = (row >= i) & (row < i + size)
        factors = [jnp.where(inside, 0.0, col) for col in picked]
        after = []
        for m in solved:
            pivots = [sum(inverse[a][n] * m[i + n : i + n + 1] for n in range(size)) for a in range(size)]
            left = m - sum(factor * pivot for factor, pivot in zip(factors, pivots))
            for n, pivot in enumerate(pivots):
                left = jnp.where(row == i + n, pivot, left)
            after.append(left)
        solved = tuple(after)
    coef, _, solver = solved
    fresh = dot(columns[:, :16], coef)
    target_ref[...] = 2.0 * fresh - gains
    owners = bands // LOCAL
    msg_ref[...] = jnp.where(
        iota((owners, 128), 1) < 64,
        target_ref[pl.ds(0, owners, stride=2), :],
        pltpu.roll(target_ref[pl.ds(1, owners, stride=2), :], 64, 1),
    )
    fresh_ref[...] = fresh
    coef_ref[...] = coef
    solver_ref[...] = solver
    start = jnp.where(lax.axis_index("band_2") == 0, 1.0, 0.0)
    primal = total(weight * (gains - fresh) ** 2)
    dual = total(jnp.where(low, weight * (fresh - start) ** 2, 0.0))
    lane = iota((8, 128), 1)
    norm_ref[...] = jnp.where(
        lane == 64, primal, jnp.where(lane == 65, dual, jnp.where(lane == 68, total(weight), 0.0))
    )


def finish_kernel(
    x_ref, target_ref, gain_ref, fresh_ref, coef_ref, solver_ref, norm_ref, msg_ref,
    coef_buf, rows_buf, gain_buf,
):
    bands = x_ref.shape[0]
    owners = bands // 2
    low = iota((bands, 128), 1) < 64
    weight = x_ref[:, 64:65]
    gain_buf[pl.ds(0, owners, stride=2), :] = gain_ref[...]
    gain_buf[pl.ds(1, owners, stride=2), :] = pltpu.roll(gain_ref[...], 64, 1)
    gains = jnp.where(low, gain_buf[...], 0.0)
    columns = basis_columns(bands)
    change = dot(solver_ref[...], weight * (gains - target_ref[...]))
    step = dot(columns[:, :16], change)
    fresh = fresh_ref[...] + step
    primal = total(weight * (gains - fresh) ** 2)
    dual = total(weight * step * step)
    lane = iota((8, 128), 1)
    norms = jnp.where(lane == 66, primal, jnp.where(lane == 67, dual, norm_ref[...]))
    row = iota((16, 128), 0)
    coef_buf[...] = jnp.where(
        row == ORDER, pltpu.roll(norms[:1], 64, 1), coef_ref[...] + change
    )
    low = iota((8, 128), 1) < 64
    packed = jnp.where(
        low, coef_buf[pl.ds(0, 8, stride=2), :], pltpu.roll(coef_buf[pl.ds(1, 8, stride=2), :], 64, 1)
    )
    for r in range(MSG_ROWS - 1):
        msg_ref[pl.ds(r, owners, stride=MSG_ROWS), :] = jnp.broadcast_to(
            packed[r : r + 1], (owners, 128)
        )
    lands = (x_ref[:, 96:97] == iota((bands, bands), 1).astype(f32)).astype(f32)
    rows_buf[...] = dot(jnp.transpose(lands), gains)
    msg_ref[pl.ds(MSG_ROWS - 1, owners, stride=MSG_ROWS), :] = jnp.where(
        iota((owners, 128), 1) < 64,
        rows_buf[pl.ds(0, owners, stride=2), :],
        pltpu.roll(rows_buf[pl.ds(1, owners, stride=2), :], 64, 1),
    )


def assemble_kernel(all_ref, delivered_ref, coef_ref):
    low = iota((16, 128), 1) < 64
    for r in range(MSG_ROWS):
        for half in range(2):
            first, second = (
                all_ref[pl.ds(MSG_ROWS * 16 * quarter + r, 16, stride=MSG_ROWS), :]
                for quarter in (2 * half, 2 * half + 1)
            )
            tiles = (
                jnp.where(low, first, pltpu.roll(second, 64, 1)),
                jnp.where(low, pltpu.roll(first, 64, 1), second),
            )
            for odd in range(2):
                if r == MSG_ROWS - 1:
                    out = delivered_ref.at[odd]
                elif 2 * r + odd < ORDER:
                    out = coef_ref.at[2 * r + odd]
                else:
                    continue
                for k in range(DIRS):
                    out[k, :, 128 * half : 128 * half + 128] = tiles[odd][2 * k : 2 * k + 2]


def norm_kernel(all_ref, norm_ref):
    owners = all_ref.shape[0] // MSG_ROWS
    sums = jnp.sum(all_ref[pl.ds(ORDER // 2, owners, stride=MSG_ROWS), :], axis=0, keepdims=True)
    sums = jnp.broadcast_to(sums, (8, 128))
    row = iota((8, 128), 0)
    norm_ref[...] = jnp.where(
        row == 0,
        pltpu.roll(sums, 64, 1),
        jnp.where(row == 1, pltpu.roll(sums, 62, 1), pltpu.roll(sums, 60, 1)),
    )


def total_kernel(own_ref, first_ref, second_ref, third_ref, out_ref):
    sums = (own_ref[...] + second_ref[...]) + (first_ref[...] + third_ref[...])
    scale = lax.axis_size(BAND) / (DIRS * lax.axis_size("dir") * 2.0 * STATIONS)
    out_ref[...] = jnp.sqrt(scale * sums[:2, :2] / own_ref[2:3, :1])


def shape(*dims):
    return jax.ShapeDtypeStruct(dims, f32)


def call(kernel, outs, *args, scratch=(), in_specs=None, limit=8 << 20):
    in_specs = in_specs or [VMEM] * len(args)
    args = [
        pltpu.with_memory_space_constraint(arg, spec.memory_space)
        for arg, spec in zip(args, in_specs)
    ]
    return pl.pallas_call(
        kernel,
        out_shape=outs,
        in_specs=in_specs,
        scratch_shapes=list(scratch),
        compiler_params=pltpu.CompilerParams(vmem_limit_bytes=limit),
        name=kernel.__name__,
    )(*args)


VMEM = pl.BlockSpec(memory_space=pltpu.VMEM)
HBM = pl.BlockSpec(memory_space=pltpu.HBM)


def exchange(message):
    return lax.all_to_all(message, BAND, split_axis=0, concat_axis=0, tiled=True)


def per_device(visibilities, sky_model, rfi_flags, destination):
    bands = LOCAL * lax.axis_size(BAND)
    columns = pltpu.VMEM((STATIONS, 128), f32)
    operator = pltpu.VMEM((PAIRS, STATIONS, STATIONS), f32)
    halves = pltpu.VMEM((PAIRS, 2, STATIONS, STATIONS), jnp.bfloat16)
    *state, message = call(
        first_kernel,
        [
            operator, operator, operator, shape(2 * PAIRS, STATIONS), shape(PAIRS, STATIONS),
            shape(bands, 128),
        ],
        rfi_flags, destination, visibilities, sky_model,
        in_specs=[HBM] * 4,
        scratch=[
            pltpu.VMEM(rfi_flags.shape, jnp.int32), pltpu.SMEM(destination.shape, jnp.int32),
            halves, halves, pltpu.VMEM((LOCAL, STATIONS, STATIONS), bf16), columns,
            pltpu.SemaphoreType.DMA((2, PAIRS + 1)),
        ],
        limit=20 << 20,
    )
    held = exchange(message)
    owners = bands // LOCAL
    message, *kept = call(
        solve_kernel,
        [
            shape(owners, 128), shape(bands, 128), shape(bands, 128), shape(16, 128),
            shape(16, 128), shape(8, 128),
        ],
        held,
    )
    rows = pltpu.VMEM((2 * PAIRS, STATIONS), f32)
    message = call(
        second_kernel, shape(owners, 128), *state, exchange(message),
        scratch=[rows, rows, columns],
    )
    target, *kept = kept
    spread = pltpu.VMEM((bands, 128), f32)
    message = call(
        finish_kernel, shape(MSG_ROWS * owners, 128), held, target, exchange(message), *kept,
        scratch=[pltpu.VMEM((16, 128), f32), spread, spread],
    )
    everything = exchange(message.reshape(owners, 1, MSG_ROWS * 128)).reshape(-1, 128)
    norms = call(norm_kernel, shape(8, 128), everything)
    count = lax.axis_size("dir")
    others = [
        lax.ppermute(norms, "dir", [(i, (i + step) % count) for i in range(count)])
        for step in range(1, count)
    ]
    delivered, coefficients = call(
        assemble_kernel,
        [shape(LOCAL, DIRS, 2, STATIONS), shape(ORDER, DIRS, 2, STATIONS)],
        everything,
    )
    norm_values = call(total_kernel, shape(2, 2), norms, *others)
    return delivered, coefficients, norm_values


def solution(mesh):
    finer = Mesh(
        mesh.devices.reshape(4, 8, 2, mesh.shape["dir"]), ("band_0", "band_1", "band_2", "dir")
    )
    return jax.shard_map(
        per_device,
        mesh=finer,
        in_specs=(
            P(BAND, "dir", None, None, None),
            P(BAND, "dir", None, None, None),
            P(BAND, None, None),
            P(BAND),
        ),
        out_specs=(P(BAND, "dir", None, None), P(None, "dir", None, None), P()),
        check_vma=False,
    )
```
